32 devices in a mesh: rows: 8 (over z, y), model: 4 (over x, core).
Axes of the slice: x: 2, y: 2, z: 4, core: 2. Of those that a mesh axis runs over, the one named last changes fastest.
Arguments:
- w_query: float32 [4096, 4096], P('rows', 'model'), may hold values from -0.125 to 0.125
- first_query: float32 [4096, 4096], P('rows', 'model'), may hold values from -6 to 6
- second_query: float32 [4096, 4096], P('rows', 'model'), may hold values from 0.1 to 10
- w_key: float32 [4096, 1024], P('rows', 'model'), may hold values from -0.125 to 0.125
- first_key: float32 [4096, 1024], P('rows', 'model'), may hold values from -6 to 6
- second_key: float32 [4096, 1024], P('rows', 'model'), may hold values from 0.1 to 10
- w_value: float32 [4096, 1024], P('rows', 'model'), may hold values from -0.125 to 0.125
- first_value: float32 [4096, 1024], P('rows', 'model'), may hold values from -6 to 6
- second_value: float32 [4096, 1024], P('rows', 'model'), may hold values from 0.1 to 10
- norm_train: float32 [4096], P(('rows', 'model')), may hold values from 0.25 to 1.75
- norm_step: float32 [4096], P(('rows', 'model')), may hold values from -0.3 to 0.3
Outputs:
- final_query: bfloat16 [4096, 4096], P(None, 'model')
- final_key: bfloat16 [4096, 1024], P(None, 'model')
- final_value: bfloat16 [4096, 1024], P(None, 'model')
- column_query: float32 [4096], P('model')
- column_key: float32 [1024], P('model')
- column_value: float32 [1024], P('model')
- serve_norm: bfloat16 [4096], replicated
- result_query: float32 [4096, 4096], P('rows', 'model')
- result_key: float32 [4096, 1024], P('rows', 'model')
- result_value: float32 [4096, 1024], P('rows', 'model')
The draws below stay inside these ranges and needn't reach their ends.
All inputs are finite; a program needn't handle non-finite values. Where the reference program divides by a largest or mean magnitude, that divisor is 1e-20 or more.
Results may differ from the reference program's by a relative error of at most 0.0004.
Values may be sent and summed in bfloat16 or wider, within the bound.
A program may use at most 64 MiB of HBM per device.

```python
import math
import jax
import jax.numpy as jnp
from jax import lax

D_MODEL = 4096
Q_DIM = 4096
KV_DIM = 1024


def strengthened(values, key, source, target, shards_of, factor):
    def block_of(dim):
        return (jnp.arange(values.shape[dim]) // (values.shape[dim] // shards_of)).reshape((-1,) + (1,) * (values.ndim - 1 - dim))

    first = jax.random.permutation(key, shards_of)[block_of(target)]
    second = (block_of(target) + shards_of // 2) % shards_of
    return jnp.where((block_of(source) == first) | (block_of(source) == second), factor * values, values)


def steps_of(rng, shape, split, low, largest):
    loudness = 1.0
    for position, parts in split:
        draws = jax.random.uniform(jax.random.fold_in(jax.random.fold_in(rng, 6), position), (parts,), jnp.float32, low / len(split), largest / len(split))
        loudness = loudness * jnp.repeat(jnp.exp(draws), shape[position] // parts).reshape((-1,) + (1,) * (len(shape) - 1 - position))
    return loudness


def gaussian(key, shape, spread, bound, cuts=(), held_as=jnp.bfloat16):
    array = jax.random.normal(key, shape, jnp.float32) * spread
    if len(cuts) > 0:
        array = steps_of(key, shape, cuts, -0.22, 0.18) * array
    return jnp.clip(array, min=-bound, max=bound).astype(held_as)


def noise_with(rng, dims, width, most, cuts, heavy, held_as=jnp.bfloat16):
    array = width * jax.random.normal(rng, dims, jnp.float32)
    if cuts:
        array = array * steps_of(rng, dims, cuts, -0.22, 0.18)
    return jnp.clip(strengthened(array, jax.random.fold_in(rng, 3), *heavy), -most, most).astype(held_as)


def setup_inputs(seed: int = 0) -> dict:
    seeds = jax.random.split(jax.random.key(seed), 12)
    w_query = noise_with(seeds[0], (D_MODEL, Q_DIM), D_MODEL ** -0.5, 0.125, ((0, 8), (1, 4)), (0, 1, 8, 2.0), jnp.float32)
    first_query = gaussian(seeds[1], (D_MODEL, Q_DIM), 1.0, 6.0, ((0, 8), (1, 4)), jnp.float32)
    second_query = jnp.clip(jnp.exp(math.log(10.0) - 4.6051702 * jax.random.uniform(seeds[2], (D_MODEL, Q_DIM), jnp.float32) ** steps_of(seeds[2], (D_MODEL, Q_DIM), ((0, 8), (1, 4)), -0.2, 0.2)), 0.1, 10.0)
    w_key = noise_with(seeds[3], (D_MODEL, KV_DIM), D_MODEL ** -0.5, 0.125, ((0, 8), (1, 4)), (0, 1, 8, 2.0), jnp.float32)
    first_key = gaussian(seeds[4], (D_MODEL, KV_DIM), 1.0, 6.0, ((0, 8), (1, 4)), jnp.float32)
    second_key = jnp.clip(jnp.exp(math.log(10.0) - 4.6051702 * jax.random.uniform(seeds[5], (D_MODEL, KV_DIM), jnp.float32) ** steps_of(seeds[5], (D_MODEL, KV_DIM), ((0, 8), (1, 4)), -0.2, 0.2)), 0.1, 10.0)
    w_value = noise_with(seeds[6], (D_MODEL, KV_DIM), D_MODEL ** -0.5, 0.125, ((0, 8), (1, 4)), (0, 1, 8, 2.0), jnp.float32)
    first_value = gaussian(seeds[7], (D_MODEL, KV_DIM), 1.0, 6.0, ((0, 8), (1, 4)), jnp.float32)
    second_value = jnp.clip(jnp.exp(math.log(10.0) - 4.6051702 * jax.random.uniform(seeds[8], (D_MODEL, KV_DIM), jnp.float32) ** steps_of(seeds[8], (D_MODEL, KV_DIM), ((0, 8), (1, 4)), -0.2, 0.2)), 0.1, 10.0)
    norm_train = jnp.clip(1.0 + 0.15 * jax.random.normal(seeds[9], (D_MODEL,), jnp.float32), 0.25, 1.75)
    norm_step = jnp.clip(jax.random.uniform(seeds[10], (D_MODEL,), jnp.float32, -0.3, 0.3) * steps_of(seeds[10], (D_MODEL,), ((0, 32),), -0.4, 0.0), -0.3, 0.3)
    return dict(w_query=w_query, first_query=first_query, second_query=second_query, w_key=w_key, first_key=first_key, second_key=second_key, w_value=w_value, first_value=first_value, second_value=second_value, norm_train=norm_train, norm_step=norm_step)


learn_rate = 0.01
decay_rate = 0.05
tiny_value = 1e-08

def reference(w_query, first_query, second_query, w_key, first_key, second_key, w_value, first_value, second_value, norm_train, norm_step):
    result_query = w_query - learn_rate * (first_query / (jnp.sqrt(second_query) + tiny_value) + decay_rate * w_query)
    result_key = w_key - learn_rate * (first_key / (jnp.sqrt(second_key) + tiny_value) + decay_rate * w_key)
    result_value = w_value - learn_rate * (first_value / (jnp.sqrt(second_value) + tiny_value) + decay_rate * w_value)
    column_query = lax.optimization_barrier(jnp.sum(jnp.abs(result_query), axis=0)) / D_MODEL
    final_query = (result_query / column_query).astype(jnp.bfloat16)
    column_key = lax.optimization_barrier(jnp.sum(jnp.abs(result_key), axis=0)) / D_MODEL
    final_key = (result_key / column_key).astype(jnp.bfloat16)
    column_value = lax.optimization_barrier(jnp.sum(jnp.abs(result_value), axis=0)) / D_MODEL
    final_value = (result_value / column_value).astype(jnp.bfloat16)
    serve_norm = (norm_train + norm_step).astype(jnp.bfloat16)
    return (final_query, final_key, final_value, column_query, column_key, column_value, serve_norm, result_query, result_key, result_value)
```

```python
import functools

import jax
import jax.numpy as jnp
from jax import lax
from jax.experimental import pallas as pl
from jax.experimental.pallas import tpu as pltpu
from jax.sharding import PartitionSpec as P

learn_rate = 0.01
decay_rate = 0.05
tiny_value = 1e-08

MESH = pl.DeviceIdType.MESH
SIDE = 2
TILE = 32


def adam(w, first, second):
    return w - learn_rate * (first / (jnp.sqrt(second) + tiny_value) + decay_rate * w)


def plain(d_model, arrays):
    *weights, norm_train, norm_step = arrays
    results = [adam(*weights[3 * i : 3 * i + 3]) for i in range(3)]
    totals = lax.psum(tuple(jnp.sum(jnp.abs(r), axis=0) for r in results), "rows")
    columns = [t / d_model for t in totals]
    finals = [
        lax.all_gather((r / c).astype(jnp.bfloat16), "rows", axis=0, tiled=True)
        for r, c in zip(results, columns)
    ]
    serve = lax.all_gather(
        (norm_train + norm_step).astype(jnp.bfloat16), ("rows", "model"), axis=0, tiled=True
    )
    return (*finals, *columns, serve, *results)


def kernel(
    n_rows, n_model, blocks, d_model,
    *refs,
):
    ins, refs = refs[:9], refs[9:]
    nt_ref, ns_ref = refs[:2]
    finals, cols, norm_out, results = refs[2:5], refs[5:8], refs[8], refs[9:12]
    bufs = refs[12:21]
    (sums, gains, in_sem, sum_send, sum_recv, gain_send, gain_recv,
     up_send, down_send, side_send, line_recv, side_recv) = refs[21:]

    line = n_rows // SIDE
    me = lax.axis_index("rows")
    col = lax.axis_index("model")
    z, y = me // SIDE, me % SIDE
    other = 1 - y
    share = bufs[0].shape[0]
    nb = len(blocks)
    lead = nb - 1

    loads = []
    for b, (a, start, width) in enumerate(blocks):
        for k in range(3):
            where = (slice(None), pl.ds(start, width))
            c = pltpu.make_async_copy(
                ins[3 * a + k].at[where], bufs[3 * a + k].at[where], in_sem.at[b, k]
            )
            c.start()
            loads.append(c)

    barrier = pltpu.get_barrier_semaphore()
    for k in range(1, n_rows):
        pl.semaphore_signal(
            barrier, inc=1, device_id={"rows": lax.rem(me + k, n_rows)}, device_id_type=MESH
        )
    for k in range(1, n_model):
        pl.semaphore_signal(
            barrier, inc=1, device_id={"model": lax.rem(col + k, n_model)}, device_id_type=MESH
        )
    gains[me, col] = nt_ref[...] + ns_ref[...]

    def step(b):
        a, start, width = blocks[b]
        for k in range(3):
            loads[3 * b + k].wait()

        def one(i, acc):
            rows = pl.ds(pl.multiple_of(i * TILE, TILE), TILE)
            where = (rows, pl.ds(start, width))
            r = adam(*(bufs[3 * a + k][where] for k in range(3)))
            results[a][where] = r
            m = jnp.abs(r).reshape(TILE // 8, 8, width)
            return acc + jnp.sum(m, axis=0)

        acc = lax.fori_loop(0, share // TILE, one, jnp.zeros((8, width), jnp.float32))
        sums[b, me] = jnp.sum(acc, axis=0, keepdims=True)

    def sum_copy(b, k):
        return pltpu.make_async_remote_copy(
            src_ref=sums.at[b, me],
            dst_ref=sums.at[b, me],
            send_sem=sum_send.at[b, k],
            recv_sem=sum_recv.at[b, k],
            device_id={"rows": lax.rem(me + k, n_rows)},
            device_id_type=MESH,
        )

    def wait_sum(b, k):
        who = lax.rem(me + n_rows - k, n_rows)
        pltpu.make_async_remote_copy(
            src_ref=sums.at[b, who],
            dst_ref=sums.at[b, who],
            send_sem=sum_send.at[b, k],
            recv_sem=sum_recv.at[b, k],
            device_id={"rows": lax.rem(me + k, n_rows)},
            device_id_type=MESH,
        ).wait_recv()

    def place(j, owner):
        a, start, width = blocks[j]
        rows = pl.ds(pl.multiple_of(owner * share, share), share)
        return finals[a].at[rows, pl.ds(start, width)]

    def to_line(zs, j, up):
        owner = zs * SIDE + (other if j == nb else y)
        part = place(min(j, lead), owner)
        return pltpu.make_async_remote_copy(
            src_ref=part,
            dst_ref=part,
            send_sem=(up_send if up else down_send).at[zs, j],
            recv_sem=line_recv.at[zs, j],
            device_id={"rows": me + (SIDE if up else -SIDE)},
            device_id_type=MESH,
        )

    def to_side(zs, j, mine=True):
        part = place(j, zs * SIDE + (y if mine else other))
        return pltpu.make_async_remote_copy(
            src_ref=part,
            dst_ref=part,
            send_sem=side_send.at[zs, j],
            recv_sem=side_recv.at[zs, j],
            device_id={"rows": z * SIDE + other},
            device_id_type=MESH,
        )

    def both_ways(zs, j):
        @pl.when(z > 0)
        def _():
            to_line(zs, j, False).start()

        @pl.when(z < line - 1)
        def _():
            to_line(zs, j, True).start()

    def gain_model(k):
        return pltpu.make_async_remote_copy(
            src_ref=gains.at[me, col],
            dst_ref=gains.at[me, col],
            send_sem=gain_send.at[k],
            recv_sem=gain_recv.at[k],
            device_id={"model": lax.rem(col + k, n_model)},
            device_id_type=MESH,
        )

    def gain_rows(k, who):
        return pltpu.make_async_remote_copy(
            src_ref=gains.at[who],
            dst_ref=gains.at[who],
            send_sem=gain_send.at[n_model + k],
            recv_sem=gain_recv.at[n_model + k],
            device_id={"rows": lax.rem(me + k, n_rows)},
            device_id_type=MESH,
        )

    order = [0, lead] + list(range(1, lead))
    for i, b in enumerate(order):
        step(b)
        if i == 0:
            pl.semaphore_wait(barrier, n_rows + n_model - 2)
        for k in range(1, n_rows):
            sum_copy(b, k).start()
    for k in range(1, n_model):
        gain_model(k).start()

    for b in order:
        a, start, width = blocks[b]
        for k in range(1, n_rows):
            wait_sum(b, k)
        total = sums[b, 0]
        for k in range(1, n_rows):
            total = total + sums[b, k]
        column = total / d_model
        cols[a][:, pl.ds(start, width)] = column
        scale = jnp.broadcast_to(1.0 / column, (TILE, width))

        def one(i, carry):
            rows = pl.ds(pl.multiple_of(i * TILE, TILE), TILE)
            there = pl.ds(pl.multiple_of(me * share + i * TILE, TILE), TILE)
            where = pl.ds(start, width)
            finals[a][there, where] = (results[a][rows, where] * scale).astype(jnp.bfloat16)
            return carry

        lax.fori_loop(0, share // TILE, one, 0)
        if b != lead:
            both_ways(z, b)
        to_side(z, b).start()
    both_ways(z, lead)

    for k in range(1, n_model):
        who = lax.rem(col + n_model - k, n_model)
        pltpu.make_async_remote_copy(
            src_ref=gains.at[me, who],
            dst_ref=gains.at[me, who],
            send_sem=gain_send.at[k],
            recv_sem=gain_recv.at[k],
            device_id={"model": lax.rem(col + k, n_model)},
            device_id_type=MESH,
        ).wait_recv()
    for k in range(1, n_rows):
        gain_rows(k, me).start()

    to_side(z, lead, False).wait_recv()
    both_ways(z, nb)

    for d in range(1, line):
        for j in range(nb + 1):

            @pl.when(z - d >= 0)
            def _():
                to_line(z - d, j, True).wait_recv()

                @pl.when(z < line - 1)
                def _():
                    to_line(z - d, j, True).start()

                if j < lead:
                    to_side(z - d, j).start()

            @pl.when(z + d < line)
            def _():
                to_line(z + d, j, False).wait_recv()

                @pl.when(z > 0)
                def _():
                    to_line(z + d, j, False).start()

                if j < lead:
                    to_side(z + d, j).start()

    for k in range(1, n_rows):
        gain_rows(k, lax.rem(me + n_rows - k, n_rows)).wait_recv()
    norm_out[...] = gains[...]

    for zs in range(line):
        for j in range(lead):
            to_side(zs, j, False).wait_recv()
    for k in range(1, n_model):
        gain_model(k).wait_send()
    for k in range(1, n_rows):
        gain_rows(k, me).wait_send()
        for b in range(nb):
            sum_copy(b, k).wait_send()
    for zs in range(line):
        for j in range(lead):
            to_side(zs, j).wait_send()
        for j in range(nb + 1):

            @pl.when((z > 0) & (z <= zs))
            def _():
                to_line(zs, j, False).wait_send()

            @pl.when((z < line - 1) & (z >= zs))
            def _():
                to_line(zs, j, True).wait_send()
    to_side(z, lead).wait_send()


def fused(n_rows, n_model, d_model, blocks, arrays):
    *weights, norm_train, norm_step = arrays
    share = weights[0].shape[0]
    widths = [weights[3 * a].shape[1] for a in range(3)]
    line, nb = n_rows // SIDE, len(blocks)
    unit = norm_train.shape[0]
    anywhere = pl.BlockSpec(memory_space=pl.ANY)
    vmem = pl.BlockSpec(memory_space=pltpu.VMEM)
    f32, dma = jnp.float32, pltpu.SemaphoreType.DMA
    out = pl.pallas_call(
        functools.partial(kernel, n_rows, n_model, blocks, d_model),
        out_shape=[
            *(pltpu.VMEM((d_model, w), jnp.bfloat16) for w in widths),
            *(pltpu.VMEM((1, w), f32) for w in widths),
            pltpu.VMEM((n_rows, n_model, 1, unit), f32),
            *(pltpu.VMEM((share, w), f32) for w in widths),
        ],
        in_specs=[anywhere] * 9 + [vmem] * 2,
        out_specs=[vmem] * 10,
        scratch_shapes=[
            *(pltpu.VMEM((share, w), f32) for w in widths for _ in range(3)),
            pltpu.VMEM((nb, n_rows, 1, blocks[0][2]), f32),
            pltpu.VMEM((n_rows, n_model, 1, unit), f32),
            dma((nb, 3)),
            dma((nb, n_rows)),
            dma((nb, n_rows)),
            dma((n_rows + n_model,)),
            dma((n_rows + n_model,)),
            dma((line, nb + 1)),
            dma((line, nb + 1)),
            dma((line, nb)),
            dma((line, nb + 1)),
            dma((line, nb)),
        ],
        compiler_params=pltpu.CompilerParams(
            collective_id=0, has_side_effects=True, vmem_limit_bytes=48 * 2**20
        ),
    )(*weights, norm_train.reshape(1, -1), norm_step.reshape(1, -1))
    finals, cols, norm, results = out[:3], out[3:6], out[6], out[7:]
    serve = norm.reshape(-1).astype(jnp.bfloat16)
    return (*finals, *(c.reshape(-1) for c in cols), serve, *results)


def solution(mesh):
    n_rows, n_model = mesh.shape["rows"], mesh.shape["model"]

    def body(*arrays):
        share = arrays[0].shape[0]
        widths = [arrays[3 * a].shape[1] for a in range(3)]
        width = min(widths)
        d_model = share * n_rows
        fits = (
            n_rows % SIDE == 0
            and 2 <= n_rows // SIDE <= 4
            and share % TILE == 0
            and width % 128 == 0
            and all(w % width == 0 for w in widths)
        )
        if not fits:
            return plain(d_model, arrays)
        blocks = tuple(
            (a, s, width) for a, w in enumerate(widths) for s in range(0, w, width)
        )
        return fused(n_rows, n_model, d_model, blocks, arrays)

    return jax.shard_map(
        body,
        mesh=mesh,
        in_specs=(P("rows", "model"),) * 9 + (P(("rows", "model")),) * 2,
        out_specs=(
            *(P(None, "model"),) * 3,
            *(P("model"),) * 3,
            P(),
            *(P("rows", "model"),) * 3,
        ),
        check_vma=False,
    )
```

```python
import functools

import jax
import jax.numpy as jnp
from jax import lax
from jax.experimental import pallas as pl
from jax.experimental.pallas import tpu as pltpu
from jax.sharding import PartitionSpec as P

learn_rate = 0.01
decay_rate = 0.05
tiny_value = 1e-08

MESH = pl.DeviceIdType.MESH
SIDE = 2
TILE = 32
PIECES = 4


def adam(w, first, second):
    return w - learn_rate * (first / (jnp.sqrt(second) + tiny_value) + decay_rate * w)


def plain(d_model, arrays):
    *weights, norm_train, norm_step = arrays
    results = [adam(*weights[3 * i : 3 * i + 3]) for i in range(3)]
    totals = lax.psum(tuple(jnp.sum(jnp.abs(r), axis=0) for r in results), "rows")
    columns = [t / d_model for t in totals]
    finals = [
        lax.all_gather((r / c).astype(jnp.bfloat16), "rows", axis=0, tiled=True)
        for r, c in zip(results, columns)
    ]
    serve = lax.all_gather(
        (norm_train + norm_step).astype(jnp.bfloat16), ("rows", "model"), axis=0, tiled=True
    )
    return (*finals, *columns, serve, *results)


def kernel(
    n_rows, n_model, blocks, d_model,
    *refs,
):
    ins, refs = refs[:9], refs[9:]
    nt_ref, ns_ref = refs[:2]
    finals, cols, norm_out, results = refs[2:5], refs[5:8], refs[8], refs[9:12]
    bufs = refs[12:21]
    (sums, gains, in_sem, sum_send, sum_recv, gain_send, gain_recv,
     up_send, down_send, side_send, line_recv, side_recv) = refs[21:]

    line = n_rows // SIDE
    me = lax.axis_index("rows")
    col = lax.axis_index("model")
    z, y = me // SIDE, me % SIDE
    other = 1 - y
    share = bufs[0].shape[0]
    nb = len(blocks)
    lead = nb - 1

    loads = []
    for b, (a, start, width) in enumerate(blocks):
        for k in range(3):
            where = (slice(None), pl.ds(start, width))
            c = pltpu.make_async_copy(
                ins[3 * a + k].at[where], bufs[3 * a + k].at[where], in_sem.at[b, k]
            )
            c.start()
            loads.append(c)

    barrier = pltpu.get_barrier_semaphore()
    for k in range(1, n_rows):
        pl.semaphore_signal(
            barrier, inc=1, device_id={"rows": lax.rem(me + k, n_rows)}, device_id_type=MESH
        )
    for k in range(1, n_model):
        pl.semaphore_signal(
            barrier, inc=1, device_id={"model": lax.rem(col + k, n_model)}, device_id_type=MESH
        )
    gains[me, col] = nt_ref[...] + ns_ref[...]

    def step(b):
        a, start, width = blocks[b]
        for k in range(3):
            loads[3 * b + k].wait()

        def one(i, acc):
            rows = pl.ds(pl.multiple_of(i * TILE, TILE), TILE)
            where = (rows, pl.ds(start, width))
            r = adam(*(bufs[3 * a + k][where] for k in range(3)))
            results[a][where] = r
            m = jnp.abs(r).reshape(TILE // 8, 8, width)
            return acc + jnp.sum(m, axis=0)

        acc = lax.fori_loop(0, share // TILE, one, jnp.zeros((8, width), jnp.float32))
        sums[b, me] = jnp.sum(acc, axis=0, keepdims=True)

    def sum_copy(b, k):
        return pltpu.make_async_remote_copy(
            src_ref=sums.at[b, me],
            dst_ref=sums.at[b, me],
            send_sem=sum_send.at[b, k],
            recv_sem=sum_recv.at[b, k],
            device_id={"rows": lax.rem(me + k, n_rows)},
            device_id_type=MESH,
        )

    def wait_sum(b, k):
        who = lax.rem(me + n_rows - k, n_rows)
        pltpu.make_async_remote_copy(
            src_ref=sums.at[b, who],
            dst_ref=sums.at[b, who],
            send_sem=sum_send.at[b, k],
            recv_sem=sum_recv.at[b, k],
            device_id={"rows": lax.rem(me + k, n_rows)},
            device_id_type=MESH,
        ).wait_recv()

    def place(j, owner):
        a, start, width = blocks[j]
        rows = pl.ds(pl.multiple_of(owner * share, share), share)
        return finals[a].at[rows, pl.ds(start, width)]

    def to_line(zs, j, up):
        owner = zs * SIDE + (other if j == nb else y)
        part = place(min(j, lead), owner)
        return pltpu.make_async_remote_copy(
            src_ref=part,
            dst_ref=part,
            send_sem=(up_send if up else down_send).at[zs, j],
            recv_sem=line_recv.at[zs, j],
            device_id={"rows": me + (SIDE if up else -SIDE)},
            device_id_type=MESH,
        )

    def to_side(zs, j, mine=True):
        part = place(j, zs * SIDE + (y if mine else other))
        return pltpu.make_async_remote_copy(
            src_ref=part,
            dst_ref=part,
            send_sem=side_send.at[zs, j],
            recv_sem=side_recv.at[zs, j],
            device_id={"rows": z * SIDE + other},
            device_id_type=MESH,
        )

    def both_ways(zs, j):
        @pl.when(z > 0)
        def _():
            to_line(zs, j, False).start()

        @pl.when(z < line - 1)
        def _():
            to_line(zs, j, True).start()

    def gain_model(k):
        return pltpu.make_async_remote_copy(
            src_ref=gains.at[me, col],
            dst_ref=gains.at[me, col],
            send_sem=gain_send.at[k],
            recv_sem=gain_recv.at[k],
            device_id={"model": lax.rem(col + k, n_model)},
            device_id_type=MESH,
        )

    def gain_rows(k, who):
        return pltpu.make_async_remote_copy(
            src_ref=gains.at[who],
            dst_ref=gains.at[who],
            send_sem=gain_send.at[n_model + k],
            recv_sem=gain_recv.at[n_model + k],
            device_id={"rows": lax.rem(me + k, n_rows)},
            device_id_type=MESH,
        )

    order = [0, lead] + list(range(1, lead))
    for i, b in enumerate(order):
        step(b)
        if i == 0:
            pl.semaphore_wait(barrier, n_rows + n_model - 2)
        for k in range(1, n_rows):
            sum_copy(b, k).start()
    for k in range(1, n_model):
        gain_model(k).start()

    for b in order:
        a, start, width = blocks[b]
        for k in range(1, n_rows):
            wait_sum(b, k)
        total = sums[b, 0]
        for k in range(1, n_rows):
            total = total + sums[b, k]
        column = total / d_model
        cols[a][:, pl.ds(start, width)] = column
        scale = jnp.broadcast_to(1.0 / column, (TILE, width))

        def one(i, carry):
            rows = pl.ds(pl.multiple_of(i * TILE, TILE), TILE)
            there = pl.ds(pl.multiple_of(me * share + i * TILE, TILE), TILE)
            where = pl.ds(start, width)
            finals[a][there, where] = (results[a][rows, where] * scale).astype(jnp.bfloat16)
            return carry

        lax.fori_loop(0, share // TILE, one, 0)
        if b != lead:
            both_ways(z, b)
        to_side(z, b).start()
    both_ways(z, lead)

    for k in range(1, n_model):
        who = lax.rem(col + n_model - k, n_model)
        pltpu.make_async_remote_copy(
            src_ref=gains.at[me, who],
            dst_ref=gains.at[me, who],
            send_sem=gain_send.at[k],
            recv_sem=gain_recv.at[k],
            device_id={"model": lax.rem(col + k, n_model)},
            device_id_type=MESH,
        ).wait_recv()
    for k in range(1, n_rows):
        gain_rows(k, me).start()

    to_side(z, lead, False).wait_recv()
    both_ways(z, nb)

    for d in range(1, line):
        for j in range(nb + 1):

            @pl.when(z - d >= 0)
            def _():
                to_line(z - d, j, True).wait_recv()

                @pl.when(z < line - 1)
                def _():
                    to_line(z - d, j, True).start()

                if j < lead:
                    to_side(z - d, j).start()

            @pl.when(z + d < line)
            def _():
                to_line(z + d, j, False).wait_recv()

                @pl.when(z > 0)
                def _():
                    to_line(z + d, j, False).start()

                if j < lead:
                    to_side(z + d, j).start()

    for k in range(1, n_rows):
        gain_rows(k, lax.rem(me + n_rows - k, n_rows)).wait_recv()
    for r in range(n_rows):
        for m in range(n_model):
            norm_out[pl.ds(r * n_model + m, 1), :] = gains[r, m]

    for zs in range(line):
        for j in range(lead):
            to_side(zs, j, False).wait_recv()
    for k in range(1, n_model):
        gain_model(k).wait_send()
    for k in range(1, n_rows):
        gain_rows(k, me).wait_send()
        for b in range(nb):
            sum_copy(b, k).wait_send()
    for zs in range(line):
        for j in range(lead):
            to_side(zs, j).wait_send()
        for j in range(nb + 1):

            @pl.when((z > 0) & (z <= zs))
            def _():
                to_line(zs, j, False).wait_send()

            @pl.when((z < line - 1) & (z >= zs))
            def _():
                to_line(zs, j, True).wait_send()
    to_side(z, lead).wait_send()


def write(pieces, *refs):
    ins, outs, sem = refs[:10], refs[10:20], refs[20]
    copies = []
    for n, (i, start, rows) in enumerate(pieces):
        where = pl.ds(start, rows)
        c = pltpu.make_async_copy(ins[i].at[where], outs[i].at[where], sem.at[n])
        c.start()
        copies.append(c)
    outs[6][...] = ins[6][...].astype(jnp.bfloat16)
    for c in copies:
        c.wait()


def fused(n_rows, n_model, d_model, blocks, arrays):
    *weights, norm_train, norm_step = arrays
    share = weights[0].shape[0]
    widths = [weights[3 * a].shape[1] for a in range(3)]
    line, nb = n_rows // SIDE, len(blocks)
    unit = norm_train.shape[0]
    anywhere = pl.BlockSpec(memory_space=pl.ANY)
    vmem = pl.BlockSpec(memory_space=pltpu.VMEM)
    f32, dma = jnp.float32, pltpu.SemaphoreType.DMA
    out = pl.pallas_call(
        functools.partial(kernel, n_rows, n_model, blocks, d_model),
        out_shape=[
            *(pltpu.VMEM((d_model, w), jnp.bfloat16) for w in widths),
            *(pltpu.VMEM((1, w), f32) for w in widths),
            pltpu.VMEM((n_rows * n_model, unit), f32),
            *(pltpu.VMEM((share, w), f32) for w in widths),
        ],
        in_specs=[anywhere] * 9 + [vmem] * 2,
        out_specs=[vmem] * 10,
        scratch_shapes=[
            *(pltpu.VMEM((share, w), f32) for w in widths for _ in range(3)),
            pltpu.VMEM((nb, n_rows, 1, blocks[0][2]), f32),
            pltpu.VMEM((n_rows, n_model, 1, unit), f32),
            dma((nb, 3)),
            dma((nb, n_rows)),
            dma((nb, n_rows)),
            dma((n_rows + n_model,)),
            dma((n_rows + n_model,)),
            dma((line, nb + 1)),
            dma((line, nb + 1)),
            dma((line, nb)),
            dma((line, nb + 1)),
            dma((line, nb)),
        ],
        compiler_params=pltpu.CompilerParams(
            collective_id=0, has_side_effects=True, vmem_limit_bytes=48 * 2**20
        ),
    )(*weights, norm_train.reshape(1, -1), norm_step.reshape(1, -1))
    pieces = []
    for i in [0, 7, 1, 2, 8, 9, 3, 4, 5]:
        rows = out[i].shape[0]
        cut = rows // PIECES if i == 0 else rows
        pieces += [(i, r, cut) for r in range(0, rows, cut)]
    done = pl.pallas_call(
        functools.partial(write, pieces),
        out_shape=[
            jax.ShapeDtypeStruct(o.shape, jnp.bfloat16 if i == 6 else o.dtype)
            for i, o in enumerate(out)
        ],
        in_specs=[vmem if i == 6 else anywhere for i in range(10)],
        out_specs=[vmem if i == 6 else anywhere for i in range(10)],
        scratch_shapes=[dma((len(pieces),))],
        compiler_params=pltpu.CompilerParams(vmem_limit_bytes=2**20),
    )(*out)
    return tuple(d.reshape(-1) if 3 <= i <= 6 else d for i, d in enumerate(done))


def solution(mesh):
    n_rows, n_model = mesh.shape["rows"], mesh.shape["model"]

    def body(*arrays):
        share = arrays[0].shape[0]
        widths = [arrays[3 * a].shape[1] for a in range(3)]
        width = min(widths)
        d_model = share * n_rows
        fits = (
            n_rows % SIDE == 0
            and 2 <= n_rows // SIDE <= 4
            and share % TILE == 0
            and width % 128 == 0
            and all(w % width == 0 for w in widths)
        )
        if not fits:
            return plain(d_model, arrays)
        blocks = tuple(
            (a, s, width) for a, w in enumerate(widths) for s in range(0, w, width)
        )
        return fused(n_rows, n_model, d_model, blocks, arrays)

    return jax.shard_map(
        body,
        mesh=mesh,
        in_specs=(P("rows", "model"),) * 9 + (P(("rows", "model")),) * 2,
        out_specs=(
            *(P(None, "model"),) * 3,
            *(P("model"),) * 3,
            P(),
            *(P("rows", "model"),) * 3,
        ),
        check_vma=False,
    )
```
